128 devices in a mesh: bank: 4 (over x_lo, core), zero: 32 (over z, y, x_hi).
Axes of the slice: x: 4 (x_hi: 2, x_lo: 2; x = x_hi * 2 + x_lo), y: 4, z: 4, core: 2. Of those that a mesh axis runs over, the one named last changes fastest.
Arguments:
- w_gate: float32 [64, 2048, 1024], P('bank', 'zero'), may hold values from -0.25 to 0.25
- avg_gate: float32 [64, 2048, 1024], P('bank', 'zero'), may hold values from -0.125 to 0.125
- w_up: float32 [64, 2048, 1024], P('bank', 'zero'), may hold values from -0.25 to 0.25
- avg_up: float32 [64, 2048, 1024], P('bank', 'zero'), may hold values from -0.125 to 0.125
- mix_share: float32 [64], P('bank'), may hold values from 0.2 to 0.8
- router_weight: float32 [2048, 64], P('zero', 'bank'), may hold values from -0.125 to 0.125
- router_gain: float32 [2048], P('zero'), may hold values from 0.25 to 1.75
Outputs:
- serve_gate: bfloat16 [64, 2048, 1024], P('bank', None, 'zero')
- serve_up: bfloat16 [64, 2048, 1024], P('bank', None, 'zero')
- scale_gate: float32 [64, 1024], P('bank', 'zero')
- scale_up: float32 [64, 1024], P('bank', 'zero')
- serve_router: bfloat16 [2048, 64], replicated
The draws below stay inside these ranges and needn't reach their ends.
All inputs are finite; a program needn't handle non-finite values. Where the reference program divides by a largest or mean magnitude, that divisor is 1e-20 or more.
Results may differ from the reference program's by a relative error of at most 0.001.
Values may be sent and summed in bfloat16 or wider, within the bound.
A program may use at most 128 MiB of HBM per device.

```python
import jax
import jax.numpy as jnp

EXPERTS = 64
D_MODEL = 2048
D_EXPERT = 1024


def strengthened(drawn, key, source, target, parts, factor):
    def block_of(position):
        return (jnp.arange(drawn.shape[position]) // (drawn.shape[position] // parts)).reshape((-1,) + (1,) * (drawn.ndim - 1 - position))

    near = jax.random.permutation(key, parts)[block_of(target)]
    second = (block_of(target) + parts // 2) % parts
    return jnp.where((block_of(source) == near) | (block_of(source) == second), factor * drawn, drawn)


def levels(rng, dims, shards, smallest, largest):
    def one(axis_at, blocks):
        steps = jax.random.uniform(jax.random.fold_in(jax.random.fold_in(rng, 6), axis_at), (blocks,), jnp.float32, smallest / len(shards), largest / len(shards))
        return jnp.repeat(jnp.exp(steps), dims[axis_at] // blocks).reshape((-1,) + (1,) * (len(dims) - axis_at - 1))

    factor_of = one(*shards[0])
    for cut in shards[1:]:
        factor_of = factor_of * one(*cut)
    return factor_of


def gaussian(key, dims, deviation, most, pieces=(), kind=jnp.bfloat16):
    array = jax.random.normal(key, dims, jnp.float32) * deviation
    if len(pieces) > 0:
        array = levels(key, dims, pieces, -0.22, 0.18) * array
    return jnp.clip(array, min=-most, max=most).astype(kind)


def heavy_noise(stream_key, extent, scale, bound, pieces, heavy, held_as=jnp.bfloat16):
    array = scale * jax.random.normal(stream_key, extent, jnp.float32)
    if pieces:
        array = array * levels(stream_key, extent, pieces, -0.22, 0.18)
    return jnp.clip(strengthened(array, jax.random.fold_in(stream_key, 3), *heavy), -bound, bound).astype(held_as)


def setup_inputs(seed: int = 0) -> dict:
    arg_keys = jax.random.split(jax.random.key(seed), 8)
    w_gate = heavy_noise(arg_keys[0], (EXPERTS, D_MODEL, D_EXPERT), D_MODEL ** -0.5, 0.25, ((0, 4), (1, 32)), (1, 2, 32, 2.75), jnp.float32)
    avg_gate = gaussian(arg_keys[1], (EXPERTS, D_MODEL, D_EXPERT), D_MODEL ** -0.5, 0.125, ((0, 4), (1, 32)), jnp.float32)
    w_up = heavy_noise(arg_keys[2], (EXPERTS, D_MODEL, D_EXPERT), D_MODEL ** -0.5, 0.25, ((0, 4), (1, 32)), (1, 2, 32, 2.75), jnp.float32)
    avg_up = gaussian(arg_keys[3], (EXPERTS, D_MODEL, D_EXPERT), D_MODEL ** -0.5, 0.125, ((0, 4), (1, 32)), jnp.float32)
    mix_share = jnp.clip(0.2 + 0.6 * jax.random.uniform(arg_keys[4], (EXPERTS,), jnp.float32) ** levels(arg_keys[4], (EXPERTS,), ((0, 4),), -0.2, 0.2), 0.2, 0.8)
    router_weight = gaussian(arg_keys[5], (D_MODEL, EXPERTS), D_MODEL ** -0.5, 0.125, ((0, 32), (1, 4)), jnp.float32)
    router_gain = jnp.clip(1.0 + 0.15 * jax.random.normal(arg_keys[6], (D_MODEL,), jnp.float32), 0.25, 1.75)
    return {"w_gate": w_gate, "avg_gate": avg_gate, "w_up": w_up, "avg_up": avg_up, "mix_share": mix_share, "router_weight": router_weight, "router_gain": router_gain}


def reference(w_gate, avg_gate, w_up, avg_up, mix_share, router_weight, router_gain):
    fresh_gate = mix_share[:, None, None] * w_gate + (1.0 - mix_share[:, None, None]) * avg_gate
    fresh_up = mix_share[:, None, None] * w_up + (1.0 - mix_share[:, None, None]) * avg_up
    scale_gate = jnp.sum(jnp.abs(fresh_gate), axis=1) / D_MODEL
    serve_gate = (fresh_gate / jnp.expand_dims(scale_gate, 1)).astype(jnp.bfloat16)
    scale_up = jnp.sum(jnp.abs(fresh_up), axis=1) / D_MODEL
    serve_up = (fresh_up / jnp.expand_dims(scale_up, 1)).astype(jnp.bfloat16)
    serve_router = (router_weight * router_gain[:, None]).astype(jnp.bfloat16)
    return serve_gate, serve_up, scale_gate, scale_up, serve_router
```

```python
import functools

import jax
import jax.numpy as jnp
from jax import lax
from jax.experimental import pallas as pl
from jax.experimental.pallas import tpu as pltpu
from jax.sharding import PartitionSpec as P

D_MODEL = 2048
EXPERTS = 16
ROWS = 64
WIDTH = 1024
PEERS = 32
SHARE = 32
F32 = jnp.float32
BF16 = jnp.bfloat16
MESH = pl.DeviceIdType.MESH


def peer_order():
    every = [(x, y, z) for z in range(4) for y in range(4) for x in range(2)][1:]
    along_x = [o for o in every if o[0]]
    along_y = [o for o in every if not o[0] and o[1]]
    along_z = [o for o in every if not o[0] and not o[1]]
    order = []
    while along_x or along_y or along_z:
        if along_x:
            order.append(along_x.pop(0))
        if along_y:
            order.append(along_y.pop(0))
        if along_z and (len(order) % 3 == 0 or not (along_x or along_y)):
            order.append(along_z.pop(0))
    return order


ORDER = peer_order()


def place(me, offset):
    x, y, z = offset
    at_z = lax.rem(me // 8 + z, 4)
    at_y = lax.rem(lax.rem(me // 2, 4) + y, 4)
    at_x = lax.rem(lax.rem(me, 2) + x, 2)
    return at_z * 8 + at_y * 2 + at_x


def wait_for(ref, sem):
    pltpu.make_async_copy(ref, ref, sem).wait()


def kernel(
    mix_ref,
    router_ref,
    gain_ref,
    w_gate,
    avg_gate,
    w_up,
    avg_up,
    out_gate,
    out_up,
    out_scale_gate,
    out_scale_up,
    out_router,
    fresh,
    other,
    part,
    part_in,
    total,
    narrow,
    landed,
    near_out,
    near_in,
    far_out,
    far_in,
    load_sem,
    part_sem,
    total_sem,
    bulk_send,
    bulk_recv,
    near_sem,
    far_sem,
):
    me = lax.axis_index("zero")
    bank = lax.axis_index("bank")
    half = lax.rem(me, 2)
    barrier = pltpu.get_barrier_semaphore()
    peers = [place(me, o) for o in ORDER]
    nearby = [
        (lax.rem(bank + b, 4), me + h * (1 - 2 * half))
        for b in range(4)
        for h in range(2)
        if (b, h) != (0, 0)
    ]
    for peer in peers:
        pl.semaphore_signal(barrier, inc=1, device_id={"zero": peer}, device_id_type=MESH)
    for to_bank, to_zero in nearby:
        pl.semaphore_signal(
            barrier, inc=1, device_id={"bank": to_bank, "zero": to_zero}, device_id_type=MESH
        )

    loads = []
    for t, (w, a) in enumerate(((w_gate, avg_gate), (w_up, avg_up))):
        for q in range(4):
            rows = pl.ds(q * 256, 256)
            pair = []
            for n, (source, target) in enumerate(((w, fresh), (a, other))):
                copy = pltpu.make_async_copy(
                    source.at[rows], target.at[t, rows], load_sem.at[t * 8 + q * 2 + n]
                )
                copy.start()
                pair.append(copy)
            loads.append(pair)

    share = router_ref[...] * gain_ref[...]
    near_out[...] = jnp.concatenate([share, share], axis=1).astype(BF16)

    for t in range(2):
        for q in range(4):
            for copy in loads[t * 4 + q]:
                copy.wait()

            def mean_step(n, carry, t=t, q=q):
                e = q * 4 + n
                mix = mix_ref[e]
                rest = 1.0 - mix
                line = t * EXPERTS + e
                rows = pl.ds(pl.multiple_of(e * ROWS, ROWS), ROWS)
                for c in range(8):
                    lanes = slice(c * 128, c * 128 + 128)
                    value = mix * fresh[t, rows, lanes] + rest * other[t, rows, lanes]
                    fresh[t, rows, lanes] = value
                    part[4 * c + line // 8, pl.ds(lax.rem(line, 8), 1), :] = jnp.sum(
                        jnp.abs(value), axis=0, keepdims=True
                    )
                return carry

            lax.fori_loop(0, 4, mean_step, 0)

    pl.semaphore_wait(barrier, len(peers) + len(nearby))

    sends = []
    for peer in peers:
        copy = pltpu.make_async_remote_copy(
            part.at[peer], part_in.at[me], part_sem.at[0], part_sem.at[1],
            device_id={"zero": peer}, device_id_type=MESH,
        )
        copy.start()
    slot = bank * 2 + half
    for to_bank, to_zero in nearby:
        pltpu.make_async_remote_copy(
            near_out, near_in.at[slot], near_sem.at[0], near_sem.at[1],
            device_id={"bank": to_bank, "zero": to_zero}, device_id_type=MESH,
        ).start()
    near_in[slot] = near_out[...]
    part_in[me] = part[me]
    wait_for(part_in.at[pl.ds(0, PEERS - 1)], part_sem.at[1])
    summed = part_in[0]
    for n in range(1, PEERS):
        summed = summed + part_in[n]
    total[me] = summed
    for peer in peers:
        pltpu.make_async_remote_copy(
            total.at[me], total.at[me], total_sem.at[0], total_sem.at[1],
            device_id={"zero": peer}, device_id_type=MESH,
        ).start()

    wait_for(near_in.at[pl.ds(0, 7)], near_sem.at[1])
    low = lax.broadcasted_iota(jnp.int32, (16, 128), 1) < 64
    for b in range(4):
        even, odd = near_in[2 * b].astype(F32), near_in[2 * b + 1].astype(F32)
        far_out[pl.ds(16 * b, 16), :] = jnp.where(low, even, odd).astype(BF16)
    for offset, peer in zip(ORDER, peers):
        if offset[0] == 0:
            pltpu.make_async_remote_copy(
                far_out, far_in.at[me // 2], far_sem.at[0], far_sem.at[1],
                device_id={"zero": peer}, device_id_type=MESH,
            ).start()
    far_in[me // 2] = far_out[...]

    wait_for(total.at[pl.ds(0, PEERS - 1)], total_sem.at[1])
    wait_for(total.at[pl.ds(0, PEERS - 1)], total_sem.at[0])
    wait_for(part.at[pl.ds(0, PEERS - 1)], part_sem.at[0])
    for out, t in ((out_scale_gate, 0), (out_scale_up, 1)):
        for g in range(2):
            tile = total[4 * (me // 4) + 2 * t + g] / D_MODEL
            shifted = pltpu.roll(tile, lax.rem(128 - SHARE * lax.rem(me, 4), 128), 1)
            out[pl.ds(8 * g, 8), :] = shifted[:, :SHARE]
    for n in range(PEERS):
        part[n] = 1.0 / (total[n] / D_MODEL)

    for t in range(2):

        def send_step(q, carry, t=t):
            c = t * 4 + q
            for j in range(8):
                for p in range(2):
                    blocks = []
                    for h in range(2):
                        e = q * 4 + p * 2 + h
                        line = t * EXPERTS + e
                        factor = part[4 * j + line // 8, pl.ds(lax.rem(line, 8), 1), :]
                        rows = pl.ds(pl.multiple_of(e * ROWS, ROWS), ROWS)
                        blocks.append(fresh[t, rows, j * 128 : j * 128 + 128] * factor)
                    block = jnp.concatenate(blocks, axis=0)
                    narrow[c, j * 128 : j * 128 + 128, p * 128 : p * 128 + 128] = block.T.astype(BF16)
            for peer in peers:
                pltpu.make_async_remote_copy(
                    narrow.at[c, pl.ds(pl.multiple_of(peer * SHARE, SHARE), SHARE)],
                    landed.at[c, me], bulk_send.at[c], bulk_recv.at[c],
                    device_id={"zero": peer}, device_id_type=MESH,
                ).start()
            landed[c, me] = narrow[c, pl.ds(pl.multiple_of(me * SHARE, SHARE), SHARE), :]
            return carry

        lax.fori_loop(0, 4, send_step, 0)

    wait_for(far_in.at[pl.ds(0, 15)], far_sem.at[1])
    for k in range(16):
        out_router[:, k * 128 : k * 128 + 128] = far_in[k]

    for t, out in ((0, out_gate), (1, out_up)):

        def place_step(q, carry, t=t, out=out):
            c = t * 4 + q
            wait_for(landed.at[c, pl.ds(0, PEERS - 1)], bulk_recv.at[c])
            for k in range(16):
                for p in range(2):
                    lanes = slice(p * 128, p * 128 + 128)
                    even, odd = landed[c, 2 * k, :, lanes], landed[c, 2 * k + 1, :, lanes]
                    e = q * 4 + p * 2
                    to = slice(k * 128, k * 128 + 128)
                    out[e, :, to] = jnp.concatenate([even[:, :64], odd[:, :64]], axis=1)
                    out[e + 1, :, to] = jnp.concatenate([even[:, 64:], odd[:, 64:]], axis=1)
            return carry

        lax.fori_loop(0, 4, place_step, 0)

    for c in range(8):
        wait_for(landed.at[c, pl.ds(0, PEERS - 1)], bulk_send.at[c])
    wait_for(near_in.at[pl.ds(0, 7)], near_sem.at[0])
    wait_for(far_in.at[pl.ds(0, 15)], far_sem.at[0])


def on_device(w_gate, avg_gate, w_up, avg_up, mix_share, router_weight, router_gain):
    flat = [a.reshape(EXPERTS * ROWS, WIDTH) for a in (w_gate, avg_gate, w_up, avg_up)]
    vmem = pl.BlockSpec(memory_space=pltpu.VMEM)
    gate, up, scale_gate, scale_up, router = pl.pallas_call(
        kernel,
        out_shape=(
            jax.ShapeDtypeStruct((EXPERTS, SHARE, D_MODEL), BF16),
            jax.ShapeDtypeStruct((EXPERTS, SHARE, D_MODEL), BF16),
            jax.ShapeDtypeStruct((EXPERTS, SHARE), F32),
            jax.ShapeDtypeStruct((EXPERTS, SHARE), F32),
            jax.ShapeDtypeStruct((4 * EXPERTS, D_MODEL), BF16),
        ),
        in_specs=[pl.BlockSpec(memory_space=pltpu.SMEM), vmem, vmem]
        + [pl.BlockSpec(memory_space=pl.ANY)] * 4,
        out_specs=(vmem,) * 5,
        scratch_shapes=[
            pltpu.VMEM((2, EXPERTS * ROWS, WIDTH), F32),
            pltpu.VMEM((2, EXPERTS * ROWS, WIDTH), F32),
            pltpu.VMEM((PEERS, 8, 128), F32),
            pltpu.VMEM((PEERS, 8, 128), F32),
            pltpu.VMEM((PEERS, 8, 128), F32),
            pltpu.VMEM((8, WIDTH, 256), BF16),
            pltpu.VMEM((8, PEERS, SHARE, 256), BF16),
            pltpu.VMEM((16, 128), BF16),
            pltpu.VMEM((8, 16, 128), BF16),
            pltpu.VMEM((64, 128), BF16),
            pltpu.VMEM((16, 64, 128), BF16),
            pltpu.SemaphoreType.DMA((16,)),
            pltpu.SemaphoreType.DMA((2,)),
            pltpu.SemaphoreType.DMA((2,)),
            pltpu.SemaphoreType.DMA((8,)),
            pltpu.SemaphoreType.DMA((8,)),
            pltpu.SemaphoreType.DMA((2,)),
            pltpu.SemaphoreType.DMA((2,)),
        ],
        compiler_params=pltpu.CompilerParams(collective_id=0, has_side_effects=True),
        name="exchange",
    )(mix_share, router_weight.T, router_gain.reshape(1, ROWS), *flat)
    return (
        jnp.swapaxes(gate, 1, 2),
        jnp.swapaxes(up, 1, 2),
        scale_gate,
        scale_up,
        router.T,
    )


def solution(mesh):
    in_specs = (
        P("bank", "zero", None),
        P("bank", "zero", None),
        P("bank", "zero", None),
        P("bank", "zero", None),
        P("bank"),
        P("zero", "bank"),
        P("zero"),
    )
    out_specs = (
        P("bank", None, "zero"),
        P("bank", None, "zero"),
        P("bank", "zero"),
        P("bank", "zero"),
        P(),
    )
    return jax.shard_map(
        on_device, mesh=mesh, in_specs=in_specs, out_specs=out_specs, check_vma=False
    )
```

```python
import functools

import jax
import jax.numpy as jnp
from jax import lax
from jax.experimental import pallas as pl
from jax.experimental.pallas import tpu as pltpu
from jax.sharding import PartitionSpec as P

D_MODEL = 2048
EXPERTS = 16
ROWS = 64
WIDTH = 1024
PEERS = 32
SHARE = 32
F32 = jnp.float32
BF16 = jnp.bfloat16
MESH = pl.DeviceIdType.MESH


def peer_order():
    every = [(x, y, z) for z in range(4) for y in range(4) for x in range(2)][1:]
    along_x = [o for o in every if o[0]]
    along_y = [o for o in every if not o[0] and o[1]]
    along_z = [o for o in every if not o[0] and not o[1]]
    order = []
    while along_x or along_y or along_z:
        if along_x:
            order.append(along_x.pop(0))
        if along_y:
            order.append(along_y.pop(0))
        if along_z and (len(order) % 3 == 0 or not (along_x or along_y)):
            order.append(along_z.pop(0))
    return order


ORDER = peer_order()
FAR_FIRST = sorted(ORDER, key=lambda o: -(2 * o[0] + min(o[1], 4 - o[1]) + min(o[2], 4 - o[2])))


def place(me, offset):
    x, y, z = offset
    at_z = lax.rem(me // 8 + z, 4)
    at_y = lax.rem(lax.rem(me // 2, 4) + y, 4)
    at_x = lax.rem(lax.rem(me, 2) + x, 2)
    return at_z * 8 + at_y * 2 + at_x


def wait_for(ref, sem):
    pltpu.make_async_copy(ref, ref, sem).wait()


def kernel(
    mix_ref,
    router_ref,
    gain_ref,
    w_gate,
    avg_gate,
    w_up,
    avg_up,
    out_gate,
    out_up,
    out_scale_gate,
    out_scale_up,
    out_router,
    fresh,
    other,
    part,
    part_in,
    total,
    narrow,
    landed,
    near_out,
    near_in,
    far_out,
    far_in,
    load_sem,
    part_sem,
    total_sem,
    bulk_send,
    bulk_recv,
    near_sem,
    far_sem,
):
    me = lax.axis_index("zero")
    bank = lax.axis_index("bank")
    half = lax.rem(me, 2)
    barrier = pltpu.get_barrier_semaphore()
    peers = [place(me, o) for o in ORDER]
    nearby = [
        (lax.rem(bank + b, 4), me + h * (1 - 2 * half))
        for b in range(4)
        for h in range(2)
        if (b, h) != (0, 0)
    ]
    for peer in peers:
        pl.semaphore_signal(barrier, inc=1, device_id={"zero": peer}, device_id_type=MESH)
    for to_bank, to_zero in nearby:
        pl.semaphore_signal(
            barrier, inc=1, device_id={"bank": to_bank, "zero": to_zero}, device_id_type=MESH
        )

    loads = []
    for t, (w, a) in enumerate(((w_gate, avg_gate), (w_up, avg_up))):
        for q in range(4):
            rows = pl.ds(q * 256, 256)
            pair = []
            for n, (source, target) in enumerate(((w, fresh), (a, other))):
                copy = pltpu.make_async_copy(
                    source.at[rows], target.at[t, rows], load_sem.at[t * 8 + q * 2 + n]
                )
                copy.start()
                pair.append(copy)
            loads.append(pair)

    share = router_ref[...] * gain_ref[...]
    near_out[...] = jnp.concatenate([share, share], axis=1).astype(BF16)

    for t in range(2):
        for q in range(4):
            for copy in loads[t * 4 + q]:
                copy.wait()

            def mean_step(n, carry, t=t, q=q):
                e = q * 4 + n
                mix = mix_ref[e]
                rest = 1.0 - mix
                line = t * EXPERTS + e
                rows = pl.ds(pl.multiple_of(e * ROWS, ROWS), ROWS)
                for c in range(8):
                    lanes = slice(c * 128, c * 128 + 128)
                    value = mix * fresh[t, rows, lanes] + rest * other[t, rows, lanes]
                    fresh[t, rows, lanes] = value
                    part[4 * c + line // 8, pl.ds(lax.rem(line, 8), 1), :] = jnp.sum(
                        jnp.abs(value), axis=0, keepdims=True
                    )
                return carry

            lax.fori_loop(0, 4, mean_step, 0)

    pl.semaphore_wait(barrier, len(peers) + len(nearby))

    sends = []
    for peer in peers:
        copy = pltpu.make_async_remote_copy(
            part.at[peer], part_in.at[me], part_sem.at[0], part_sem.at[1],
            device_id={"zero": peer}, device_id_type=MESH,
        )
        copy.start()
    slot = bank * 2 + half
    for to_bank, to_zero in nearby:
        pltpu.make_async_remote_copy(
            near_out, near_in.at[slot], near_sem.at[0], near_sem.at[1],
            device_id={"bank": to_bank, "zero": to_zero}, device_id_type=MESH,
        ).start()
    near_in[slot] = near_out[...]
    part_in[me] = part[me]
    wait_for(part_in.at[pl.ds(0, PEERS - 1)], part_sem.at[1])
    summed = part_in[0]
    for n in range(1, PEERS):
        summed = summed + part_in[n]
    total[me] = summed
    for peer in peers:
        pltpu.make_async_remote_copy(
            total.at[me], total.at[me], total_sem.at[0], total_sem.at[1],
            device_id={"zero": peer}, device_id_type=MESH,
        ).start()

    wait_for(near_in.at[pl.ds(0, 7)], near_sem.at[1])
    low = lax.broadcasted_iota(jnp.int32, (16, 128), 1) < 64
    for b in range(4):
        even, odd = near_in[2 * b].astype(F32), near_in[2 * b + 1].astype(F32)
        far_out[pl.ds(16 * b, 16), :] = jnp.where(low, even, odd).astype(BF16)
    for offset, peer in zip(ORDER, peers):
        if offset[0] == 0:
            pltpu.make_async_remote_copy(
                far_out, far_in.at[me // 2], far_sem.at[0], far_sem.at[1],
                device_id={"zero": peer}, device_id_type=MESH,
            ).start()
    far_in[me // 2] = far_out[...]

    wait_for(total.at[pl.ds(0, PEERS - 1)], total_sem.at[1])
    wait_for(total.at[pl.ds(0, PEERS - 1)], total_sem.at[0])
    wait_for(part.at[pl.ds(0, PEERS - 1)], part_sem.at[0])
    for out, t in ((out_scale_gate, 0), (out_scale_up, 1)):
        for g in range(2):
            tile = total[4 * (me // 4) + 2 * t + g] / D_MODEL
            shifted = pltpu.roll(tile, lax.rem(128 - SHARE * lax.rem(me, 4), 128), 1)
            out[pl.ds(8 * g, 8), :] = shifted[:, :SHARE]
    for n in range(PEERS):
        part[n] = 1.0 / (total[n] / D_MODEL)

    for t in range(2):

        def send_step(q, carry, t=t, order=peers):
            c = t * 4 + q
            for j in range(8):
                for p in range(2):
                    blocks = []
                    for h in range(2):
                        e = q * 4 + p * 2 + h
                        line = t * EXPERTS + e
                        factor = part[4 * j + line // 8, pl.ds(lax.rem(line, 8), 1), :]
                        rows = pl.ds(pl.multiple_of(e * ROWS, ROWS), ROWS)
                        blocks.append(fresh[t, rows, j * 128 : j * 128 + 128] * factor)
                    block = jnp.concatenate(blocks, axis=0)
                    narrow[c, j * 128 : j * 128 + 128, p * 128 : p * 128 + 128] = block.T.astype(BF16)
            for peer in order:
                pltpu.make_async_remote_copy(
                    narrow.at[c, pl.ds(pl.multiple_of(peer * SHARE, SHARE), SHARE)],
                    landed.at[c, me], bulk_send.at[c], bulk_recv.at[c],
                    device_id={"zero": peer}, device_id_type=MESH,
                ).start()
            landed[c, me] = narrow[c, pl.ds(pl.multiple_of(me * SHARE, SHARE), SHARE), :]
            return carry

        lax.fori_loop(0, 4 - t, send_step, 0)
        if t == 1:
            send_step(3, 0, order=[place(me, o) for o in FAR_FIRST])

    wait_for(far_in.at[pl.ds(0, 15)], far_sem.at[1])
    for k in range(16):
        out_router[:, k * 128 : k * 128 + 128] = far_in[k]

    for t, out in ((0, out_gate), (1, out_up)):

        def place_step(q, carry, t=t, out=out):
            c = t * 4 + q
            wait_for(landed.at[c, pl.ds(0, PEERS - 1)], bulk_recv.at[c])
            for k in range(16):
                for p in range(2):
                    lanes = slice(p * 128, p * 128 + 128)
                    even, odd = landed[c, 2 * k, :, lanes], landed[c, 2 * k + 1, :, lanes]
                    e = q * 4 + p * 2
                    to = slice(k * 128, k * 128 + 128)
                    out[e, :, to] = jnp.concatenate([even[:, :64], odd[:, :64]], axis=1)
                    out[e + 1, :, to] = jnp.concatenate([even[:, 64:], odd[:, 64:]], axis=1)
            return carry

        lax.fori_loop(0, 4, place_step, 0)

    for c in range(8):
        wait_for(landed.at[c, pl.ds(0, PEERS - 1)], bulk_send.at[c])
    wait_for(near_in.at[pl.ds(0, 7)], near_sem.at[0])
    wait_for(far_in.at[pl.ds(0, 15)], far_sem.at[0])


def write_out(*refs):
    sources, targets, sems = refs[:5], refs[5:10], refs[10]
    copies = [pltpu.make_async_copy(*pair, sems.at[n]) for n, pair in enumerate(zip(sources, targets))]
    for copy in copies:
        copy.start()
    for copy in copies:
        copy.wait()


def on_device(w_gate, avg_gate, w_up, avg_up, mix_share, router_weight, router_gain):
    flat = [a.reshape(EXPERTS * ROWS, WIDTH) for a in (w_gate, avg_gate, w_up, avg_up)]
    vmem = pl.BlockSpec(memory_space=pltpu.VMEM)
    results = (
        ((EXPERTS, SHARE, D_MODEL), BF16),
        ((EXPERTS, SHARE, D_MODEL), BF16),
        ((EXPERTS, SHARE), F32),
        ((EXPERTS, SHARE), F32),
        ((4 * EXPERTS, D_MODEL), BF16),
    )
    held = pl.pallas_call(
        kernel,
        out_shape=tuple(pltpu.VMEM(*r) for r in results),
        in_specs=[pl.BlockSpec(memory_space=pltpu.SMEM), vmem, vmem]
        + [pl.BlockSpec(memory_space=pltpu.HBM)] * 4,
        out_specs=(vmem,) * 5,
        scratch_shapes=[
            pltpu.VMEM((2, EXPERTS * ROWS, WIDTH), F32),
            pltpu.VMEM((2, EXPERTS * ROWS, WIDTH), F32),
            pltpu.VMEM((PEERS, 8, 128), F32),
            pltpu.VMEM((PEERS, 8, 128), F32),
            pltpu.VMEM((PEERS, 8, 128), F32),
            pltpu.VMEM((8, WIDTH, 256), BF16),
            pltpu.VMEM((8, PEERS, SHARE, 256), BF16),
            pltpu.VMEM((16, 128), BF16),
            pltpu.VMEM((8, 16, 128), BF16),
            pltpu.VMEM((64, 128), BF16),
            pltpu.VMEM((16, 64, 128), BF16),
            pltpu.SemaphoreType.DMA((16,)),
            pltpu.SemaphoreType.DMA((2,)),
            pltpu.SemaphoreType.DMA((2,)),
            pltpu.SemaphoreType.DMA((8,)),
            pltpu.SemaphoreType.DMA((8,)),
            pltpu.SemaphoreType.DMA((2,)),
            pltpu.SemaphoreType.DMA((2,)),
        ],
        compiler_params=pltpu.CompilerParams(
            collective_id=0, has_side_effects=True, vmem_limit_bytes=58 * 1024 * 1024
        ),
        name="exchange",
    )(mix_share, router_weight.T, router_gain.reshape(1, ROWS), *flat)
    gate, up, scale_gate, scale_up, router = pl.pallas_call(
        write_out,
        out_shape=tuple(pltpu.HBM(*r) for r in results),
        in_specs=[vmem] * len(results),
        out_specs=(pl.BlockSpec(memory_space=pltpu.HBM),) * len(results),
        scratch_shapes=[pltpu.SemaphoreType.DMA((len(results),))],
        compiler_params=pltpu.CompilerParams(vmem_limit_bytes=16 * 1024 * 1024),
        name="write_out",
    )(*(pltpu.with_memory_space_constraint(a, pltpu.VMEM) for a in held))
    return (
        jnp.swapaxes(gate, 1, 2),
        jnp.swapaxes(up, 1, 2),
        scale_gate,
        scale_up,
        router.T,
    )


def solution(mesh):
    in_specs = (
        P("bank", "zero", None),
        P("bank", "zero", None),
        P("bank", "zero", None),
        P("bank", "zero", None),
        P("bank"),
        P("zero", "bank"),
        P("zero"),
    )
    out_specs = (
        P("bank", None, "zero"),
        P("bank", None, "zero"),
        P("bank", "zero"),
        P("bank", "zero"),
        P(),
    )
    return jax.shard_map(
        on_device, mesh=mesh, in_specs=in_specs, out_specs=out_specs, check_vma=False
    )
```

```python
import functools

import jax
import jax.numpy as jnp
from jax import lax
from jax.experimental import pallas as pl
from jax.experimental.pallas import tpu as pltpu
from jax.sharding import PartitionSpec as P

D_MODEL = 2048
EXPERTS = 16
ROWS = 64
WIDTH = 1024
PEERS = 32
SHARE = 32
EARLY = 1
BEFORE = 3
F32 = jnp.float32
BF16 = jnp.bfloat16
MESH = pl.DeviceIdType.MESH


def peer_order():
    every = [(x, y, z) for z in range(4) for y in range(4) for x in range(2)][1:]
    along_x = [o for o in every if o[0]]
    along_y = [o for o in every if not o[0] and o[1]]
    along_z = [o for o in every if not o[0] and not o[1]]
    order = []
    while along_x or along_y or along_z:
        if along_x:
            order.append(along_x.pop(0))
        if along_y:
            order.append(along_y.pop(0))
        if along_z and (len(order) % 3 == 0 or not (along_x or along_y)):
            order.append(along_z.pop(0))
    return order


ORDER = peer_order()
FAR_FIRST = sorted(ORDER, key=lambda o: -(2 * o[0] + min(o[1], 4 - o[1]) + min(o[2], 4 - o[2])))


def place(me, offset):
    x, y, z = offset
    at_z = lax.rem(me // 8 + z, 4)
    at_y = lax.rem(lax.rem(me // 2, 4) + y, 4)
    at_x = lax.rem(lax.rem(me, 2) + x, 2)
    return at_z * 8 + at_y * 2 + at_x


def wait_for(ref, sem):
    pltpu.make_async_copy(ref, ref, sem).wait()


def kernel(
    mix_ref,
    router_ref,
    gain_ref,
    w_gate,
    avg_gate,
    w_up,
    avg_up,
    out_gate,
    out_up,
    out_scale_gate,
    out_scale_up,
    out_router,
    fresh,
    other,
    part,
    part_in,
    total,
    inverse,
    square,
    columns,
    early_out,
    early_in,
    narrow,
    landed,
    near_out,
    near_in,
    far_out,
    far_in,
    load_sem,
    part_send,
    part_recv,
    total_send,
    total_recv,
    early_send,
    early_recv,
    bulk_send,
    bulk_recv,
    near_sem,
    far_sem,
):
    me = lax.axis_index("zero")
    bank = lax.axis_index("bank")
    half = lax.rem(me, 2)
    barrier = pltpu.get_barrier_semaphore()
    peers = [place(me, o) for o in ORDER]
    far_first = [place(me, o) for o in FAR_FIRST]
    nearby = [
        (lax.rem(bank + b, 4), me + h * (1 - 2 * half))
        for b in range(4)
        for h in range(2)
        if (b, h) != (0, 0)
    ]
    for peer in far_first:
        pl.semaphore_signal(barrier, inc=1, device_id={"zero": peer}, device_id_type=MESH)
    for to_bank, to_zero in nearby:
        pl.semaphore_signal(
            barrier, inc=1, device_id={"bank": to_bank, "zero": to_zero}, device_id_type=MESH
        )

    loads = []
    for t, (w, a) in enumerate(((w_gate, avg_gate), (w_up, avg_up))):
        for q in range(4):
            rows = pl.ds(q * 256, 256)
            for n, (source, target) in enumerate(((w, fresh), (a, other))):
                copy = pltpu.make_async_copy(
                    source.at[rows], target.at[t, rows], load_sem.at[t * 8 + q * 2 + n]
                )
                copy.start()
                loads.append(copy)

    share = router_ref[...] * gain_ref[...]
    near_out[...] = jnp.concatenate([share, share], axis=1).astype(BF16)

    def mean(t, first=0, last=4):
        for q in range(first, last):
            for copy in loads[t * 8 + q * 2 : t * 8 + q * 2 + 2]:
                copy.wait()

            def mean_step(n, carry, q=q):
                e = q * 4 + n
                mix = mix_ref[e]
                rest = 1.0 - mix
                rows = pl.ds(pl.multiple_of(e * ROWS, ROWS), ROWS)
                for c in range(8):
                    lanes = slice(c * 128, c * 128 + 128)
                    value = mix * fresh[t, rows, lanes] + rest * other[t, rows, lanes]
                    fresh[t, rows, lanes] = value
                    part[t, 4 * c + q, pl.ds(n, 1), :] = jnp.sum(
                        jnp.abs(value), axis=0, keepdims=True
                    )
                return carry

            lax.fori_loop(0, 4, mean_step, 0)

    def share_parts(t):
        for peer in far_first:
            pltpu.make_async_remote_copy(
                part.at[t, peer], part_in.at[t, me], part_send.at[t], part_recv.at[t],
                device_id={"zero": peer}, device_id_type=MESH,
            ).start()
        part_in[t, me] = part[t, me]

    def share_totals(t):
        wait_for(part_in.at[t, pl.ds(0, PEERS - 1)], part_recv.at[t])
        summed = part_in[t, 0]
        for n in range(1, PEERS):
            summed = summed + part_in[t, n]
        total[t, me] = summed
        for peer in far_first:
            pltpu.make_async_remote_copy(
                total.at[t, me], total.at[t, me], total_send.at[t], total_recv.at[t],
                device_id={"zero": peer}, device_id_type=MESH,
            ).start()

    def take_totals(t, out):
        wait_for(total.at[t, pl.ds(0, PEERS - 1)], total_recv.at[t])
        wait_for(total.at[t, pl.ds(0, PEERS - 1)], total_send.at[t])
        for n in range(PEERS):
            inverse[t, n] = 1.0 / (total[t, n] / D_MODEL)
        turn = lax.rem(128 - SHARE * lax.rem(me, 4), 128)
        for g in range(4):
            tile = total[t, 4 * (me // 4) + g] / D_MODEL
            out[pl.ds(4 * g, 4), :] = pltpu.roll(tile, turn, 1)[:, :SHARE]

    def turned(t, pair, j, scaled):
        blocks = []
        for h in range(2):
            e = pair * 2 + h
            rows = pl.ds(pl.multiple_of(e * ROWS, ROWS), ROWS)
            block = fresh[t, rows, j * 128 : j * 128 + 128]
            if scaled:
                block = block * inverse[t, 4 * j + e // 4, pl.ds(lax.rem(e, 4), 1), :]
            blocks.append(block)
        return jnp.concatenate(blocks, axis=0).T

    def early_unit(u):
        for j in range(8):
            early_out[u, j * 128 : j * 128 + 128, :] = turned(0, u, j, False)
        early_in[u, me] = early_out[u, pl.ds(pl.multiple_of(me * SHARE, SHARE), SHARE), :]

    def early_piece(u, h):
        for peer in peers:
            pltpu.make_async_remote_copy(
                early_out.at[u, pl.ds(pl.multiple_of(peer * SHARE + h * 8, 8), 8)],
                early_in.at[u, me, pl.ds(h * 8, 8)],
                early_send.at[4 * u + h], early_recv.at[4 * u + h],
                device_id={"zero": peer}, device_id_type=MESH,
            ).start()

    def bulk_unit(t, pair, order):
        u = t * 8 + pair
        for j in range(8):
            narrow[u, j * 128 : j * 128 + 128, :] = turned(t, pair, j, True).astype(BF16)
        for peer in order:
            pltpu.make_async_remote_copy(
                narrow.at[u, pl.ds(pl.multiple_of(peer * SHARE, SHARE), SHARE)],
                landed.at[u, me], bulk_send.at[u], bulk_recv.at[u],
                device_id={"zero": peer}, device_id_type=MESH,
            ).start()
        landed[u, me] = narrow[u, pl.ds(pl.multiple_of(me * SHARE, SHARE), SHARE), :]

    def bulk(t, start, stop):
        def step(pair, carry):
            bulk_unit(t, pair, peers)
            return carry

        lax.fori_loop(start, stop, step, 0)

    mean(0, 0, 1)
    if EARLY:
        early_unit(0)
    mean(0, 1, 4)
    pl.semaphore_wait(barrier, len(peers) + len(nearby))
    share_parts(0)
    slot = bank * 2 + half
    for to_bank, to_zero in nearby:
        pltpu.make_async_remote_copy(
            near_out, near_in.at[slot], near_sem.at[0], near_sem.at[1],
            device_id={"bank": to_bank, "zero": to_zero}, device_id_type=MESH,
        ).start()
    near_in[slot] = near_out[...]
    pieces = [(u, h) for u in range(EARLY) for h in range(4)]
    for piece in pieces[:BEFORE]:
        early_piece(*piece)
    mean(1)
    share_totals(0)
    share_parts(1)
    for u in range(1, EARLY):
        early_unit(u)
    for piece in pieces[BEFORE:]:
        early_piece(*piece)

    wait_for(near_in.at[pl.ds(0, 7)], near_sem.at[1])
    low = lax.broadcasted_iota(jnp.int32, (16, 128), 1) < 64
    for b in range(4):
        even, odd = near_in[2 * b].astype(F32), near_in[2 * b + 1].astype(F32)
        far_out[pl.ds(16 * b, 16), :] = jnp.where(low, even, odd).astype(BF16)
    for offset, peer in zip(ORDER, peers):
        if offset[0] == 0:
            pltpu.make_async_remote_copy(
                far_out, far_in.at[me // 2], far_sem.at[0], far_sem.at[1],
                device_id={"zero": peer}, device_id_type=MESH,
            ).start()
    far_in[me // 2] = far_out[...]

    take_totals(0, out_scale_gate)
    bulk(0, EARLY, EARLY + 2)
    share_totals(1)
    bulk(0, EARLY + 2, 8)
    take_totals(1, out_scale_up)
    bulk(1, 0, 7)
    bulk_unit(1, 7, far_first)

    wait_for(far_in.at[pl.ds(0, 15)], far_sem.at[1])
    for k in range(16):
        out_router[:, k * 128 : k * 128 + 128] = far_in[k]

    if EARLY:
        square[...] = jnp.zeros_like(square)
        square[0:4, :] = inverse[0, 4 * (me // 4)]
        columns[...] = square[...].T
        mine = columns[pl.ds(pl.multiple_of(SHARE * lax.rem(me, 4), SHARE), SHARE), :]
    for u in range(EARLY):
        for h in range(4):
            wait_for(early_in.at[u, pl.ds(0, PEERS - 1), pl.ds(0, 8)], early_recv.at[4 * u + h])
        for k in range(16):
            even, odd = early_in[u, 2 * k], early_in[u, 2 * k + 1]
            to = slice(k * 128, k * 128 + 128)
            for h, lanes in ((0, slice(0, 64)), (1, slice(64, 128))):
                e = 2 * u + h
                row = jnp.concatenate([even[:, lanes], odd[:, lanes]], axis=1)
                out_gate[e, :, to] = (row * mine[:, e : e + 1]).astype(BF16)

    for t, out in ((0, out_gate), (1, out_up)):

        def place_step(pair, carry, t=t, out=out):
            u = t * 8 + pair
            wait_for(landed.at[u, pl.ds(0, PEERS - 1)], bulk_recv.at[u])
            for k in range(16):
                even, odd = landed[u, 2 * k], landed[u, 2 * k + 1]
                to = slice(k * 128, k * 128 + 128)
                out[pair * 2, :, to] = jnp.concatenate([even[:, :64], odd[:, :64]], axis=1)
                out[pair * 2 + 1, :, to] = jnp.concatenate([even[:, 64:], odd[:, 64:]], axis=1)
            return carry

        lax.fori_loop(EARLY * (1 - t), 8, place_step, 0)

    for u, h in pieces:
        wait_for(early_in.at[u, pl.ds(0, PEERS - 1), pl.ds(0, 8)], early_send.at[4 * u + h])
    for u in range(EARLY, 16):
        wait_for(landed.at[u, pl.ds(0, PEERS - 1)], bulk_send.at[u])
    for t in range(2):
        wait_for(part_in.at[t, pl.ds(0, PEERS - 1)], part_send.at[t])
    wait_for(near_in.at[pl.ds(0, 7)], near_sem.at[0])
    wait_for(far_in.at[pl.ds(0, 15)], far_sem.at[0])


def write_out(*refs):
    sources, targets, sems = refs[:5], refs[5:10], refs[10]
    copies = [pltpu.make_async_copy(*pair, sems.at[n]) for n, pair in enumerate(zip(sources, targets))]
    for copy in copies:
        copy.start()
    for copy in copies:
        copy.wait()


def on_device(w_gate, avg_gate, w_up, avg_up, mix_share, router_weight, router_gain):
    flat = [a.reshape(EXPERTS * ROWS, WIDTH) for a in (w_gate, avg_gate, w_up, avg_up)]
    vmem = pl.BlockSpec(memory_space=pltpu.VMEM)
    results = (
        ((EXPERTS, SHARE, D_MODEL), BF16),
        ((EXPERTS, SHARE, D_MODEL), BF16),
        ((EXPERTS, SHARE), F32),
        ((EXPERTS, SHARE), F32),
        ((4 * EXPERTS, D_MODEL), BF16),
    )
    held = pl.pallas_call(
        kernel,
        out_shape=tuple(pltpu.VMEM(*r) for r in results),
        in_specs=[pl.BlockSpec(memory_space=pltpu.SMEM), vmem, vmem]
        + [pl.BlockSpec(memory_space=pltpu.HBM)] * 4,
        out_specs=(vmem,) * 5,
        scratch_shapes=[
            pltpu.VMEM((2, EXPERTS * ROWS, WIDTH), F32),
            pltpu.VMEM((2, EXPERTS * ROWS, WIDTH), F32),
            pltpu.VMEM((2, PEERS, 4, 128), F32),
            pltpu.VMEM((2, PEERS, 4, 128), F32),
            pltpu.VMEM((2, PEERS, 4, 128), F32),
            pltpu.VMEM((2, PEERS, 4, 128), F32),
            pltpu.VMEM((128, 128), F32),
            pltpu.VMEM((128, 128), F32),
            pltpu.VMEM((max(EARLY, 1), WIDTH, 128), F32),
            pltpu.VMEM((max(EARLY, 1), PEERS, SHARE, 128), F32),
            pltpu.VMEM((16, WIDTH, 128), BF16),
            pltpu.VMEM((16, PEERS, SHARE, 128), BF16),
            pltpu.VMEM((16, 128), BF16),
            pltpu.VMEM((8, 16, 128), BF16),
            pltpu.VMEM((64, 128), BF16),
            pltpu.VMEM((16, 64, 128), BF16),
            pltpu.SemaphoreType.DMA((16,)),
            pltpu.SemaphoreType.DMA((2,)),
            pltpu.SemaphoreType.DMA((2,)),
            pltpu.SemaphoreType.DMA((2,)),
            pltpu.SemaphoreType.DMA((2,)),
            pltpu.SemaphoreType.DMA((max(4 * EARLY, 1),)),
            pltpu.SemaphoreType.DMA((max(4 * EARLY, 1),)),
            pltpu.SemaphoreType.DMA((16,)),
            pltpu.SemaphoreType.DMA((16,)),
            pltpu.SemaphoreType.DMA((2,)),
            pltpu.SemaphoreType.DMA((2,)),
        ],
        compiler_params=pltpu.CompilerParams(
            collective_id=0, has_side_effects=True, vmem_limit_bytes=58 * 1024 * 1024
        ),
        name="exchange",
    )(mix_share, router_weight.T, router_gain.reshape(1, ROWS), *flat)
    gate, up, scale_gate, scale_up, router = pl.pallas_call(
        write_out,
        out_shape=tuple(pltpu.HBM(*r) for r in results),
        in_specs=[vmem] * len(results),
        out_specs=(pl.BlockSpec(memory_space=pltpu.HBM),) * len(results),
        scratch_shapes=[pltpu.SemaphoreType.DMA((len(results),))],
        compiler_params=pltpu.CompilerParams(vmem_limit_bytes=16 * 1024 * 1024),
        name="write_out",
    )(*(pltpu.with_memory_space_constraint(a, pltpu.VMEM) for a in held))
    return (
        jnp.swapaxes(gate, 1, 2),
        jnp.swapaxes(up, 1, 2),
        scale_gate,
        scale_up,
        router.T,
    )


def solution(mesh):
    in_specs = (
        P("bank", "zero", None),
        P("bank", "zero", None),
        P("bank", "zero", None),
        P("bank", "zero", None),
        P("bank"),
        P("zero", "bank"),
        P("zero"),
    )
    out_specs = (
        P("bank", None, "zero"),
        P("bank", None, "zero"),
        P("bank", "zero"),
        P("bank", "zero"),
        P(),
    )
    return jax.shard_map(
        on_device, mesh=mesh, in_specs=in_specs, out_specs=out_specs, check_vma=False
    )
```

```python
import functools

import jax
import jax.numpy as jnp
from jax import lax
from jax.experimental import pallas as pl
from jax.experimental.pallas import tpu as pltpu
from jax.sharding import PartitionSpec as P

D_MODEL = 2048
EXPERTS = 16
ROWS = 64
WIDTH = 1024
PEERS = 32
SHARE = 32
EARLY = 1
F32 = jnp.float32
BF16 = jnp.bfloat16
MESH = pl.DeviceIdType.MESH


def peer_order():
    every = [(x, y, z) for z in range(4) for y in range(4) for x in range(2)][1:]
    along_x = [o for o in every if o[0]]
    along_y = [o for o in every if not o[0] and o[1]]
    along_z = [o for o in every if not o[0] and not o[1]]
    order = []
    while along_x or along_y or along_z:
        if along_x:
            order.append(along_x.pop(0))
        if along_y:
            order.append(along_y.pop(0))
        if along_z and (len(order) % 3 == 0 or not (along_x or along_y)):
            order.append(along_z.pop(0))
    return order


ORDER = peer_order()
FAR_FIRST = sorted(ORDER, key=lambda o: -(2 * o[0] + min(o[1], 4 - o[1]) + min(o[2], 4 - o[2])))


def place(me, offset):
    x, y, z = offset
    at_z = lax.rem(me // 8 + z, 4)
    at_y = lax.rem(lax.rem(me // 2, 4) + y, 4)
    at_x = lax.rem(lax.rem(me, 2) + x, 2)
    return at_z * 8 + at_y * 2 + at_x


def wait_for(ref, sem):
    pltpu.make_async_copy(ref, ref, sem).wait()


def kernel(
    mix_ref,
    router_ref,
    gain_ref,
    w_gate,
    avg_gate,
    w_up,
    avg_up,
    out_gate,
    out_up,
    out_scale_gate,
    out_scale_up,
    out_router,
    fresh,
    other,
    part,
    part_in,
    total,
    inverse,
    square,
    columns,
    early_out,
    early_in,
    narrow,
    landed,
    near_out,
    near_in,
    far_out,
    far_in,
    load_sem,
    part_send,
    part_recv,
    total_send,
    total_recv,
    early_send,
    early_recv,
    bulk_send,
    bulk_recv,
    near_sem,
    far_sem,
):
    me = lax.axis_index("zero")
    bank = lax.axis_index("bank")
    half = lax.rem(me, 2)
    tile = me // 2
    barrier = pltpu.get_barrier_semaphore()
    peers = [place(me, o) for o in ORDER]
    far_first = [place(me, o) for o in FAR_FIRST]
    nearby = [
        (lax.rem(bank + b, 4), me + h * (1 - 2 * half))
        for b in range(4)
        for h in range(2)
        if (b, h) != (0, 0)
    ]
    plane = [place(me, o) for o in FAR_FIRST if o[0] == 0]
    across = [place(me, o) for o in FAR_FIRST if o[0] == 1]
    for peer in plane:
        pl.semaphore_signal(barrier, inc=1, device_id={"zero": peer}, device_id_type=MESH)
    for to_bank, to_zero in nearby:
        pl.semaphore_signal(
            barrier, inc=1, device_id={"bank": to_bank, "zero": to_zero}, device_id_type=MESH
        )

    loads = []
    for t, (w, a) in enumerate(((w_gate, avg_gate), (w_up, avg_up))):
        for q in range(4):
            rows = pl.ds(q * 256, 256)
            for n, (source, target) in enumerate(((w, fresh), (a, other))):
                copy = pltpu.make_async_copy(
                    source.at[rows], target.at[t, rows], load_sem.at[t * 8 + q * 2 + n]
                )
                copy.start()
                loads.append(copy)

    share = router_ref[...] * gain_ref[...]
    near_out[...] = jnp.concatenate([share, share], axis=1).astype(BF16)

    def mean(t, first=0, last=4):
        for q in range(first, last):
            for copy in loads[t * 8 + q * 2 : t * 8 + q * 2 + 2]:
                copy.wait()

            def mean_step(n, carry, q=q):
                e = q * 4 + n
                mix = mix_ref[e]
                rest = 1.0 - mix
                rows = pl.ds(pl.multiple_of(e * ROWS, ROWS), ROWS)
                for c in range(8):
                    lanes = slice(c * 128, c * 128 + 128)
                    value = mix * fresh[t, rows, lanes] + rest * other[t, rows, lanes]
                    fresh[t, rows, lanes] = value
                    part[t, 2 * c + e // 8, pl.ds(lax.rem(e, 8), 1), :] = jnp.sum(
                        jnp.abs(value), axis=0, keepdims=True
                    )
                return carry

            lax.fori_loop(0, 4, mean_step, 0)

    def share_parts(t):
        for peer in plane:
            pltpu.make_async_remote_copy(
                part.at[t, peer // 2], part_in.at[t, tile], part_send.at[t], part_recv.at[t],
                device_id={"zero": peer}, device_id_type=MESH,
            ).start()
        part_in[t, tile] = part[t, tile]

    def share_totals(t):
        wait_for(part_in.at[t, pl.ds(0, 15)], part_recv.at[t])
        summed = part_in[t, 0]
        for n in range(1, 16):
            summed = summed + part_in[t, n]
        total[t, me] = summed
        for peer in far_first:
            pltpu.make_async_remote_copy(
                total.at[t, me], total.at[t, me], total_send.at[t], total_recv.at[t],
                device_id={"zero": peer}, device_id_type=MESH,
            ).start()

    def take_totals(t, out):
        wait_for(total.at[t, pl.ds(0, PEERS - 1)], total_recv.at[t])
        wait_for(total.at[t, pl.ds(0, PEERS - 1)], total_send.at[t])
        for n in range(16):
            total[t, 2 * n] = (total[t, 2 * n] + total[t, 2 * n + 1]) / D_MODEL
            inverse[t, n] = 1.0 / total[t, 2 * n]
        turn = lax.rem(128 - SHARE * lax.rem(me, 4), 128)
        for g in range(2):
            scale = total[t, 2 * (2 * (me // 4) + g)]
            out[pl.ds(8 * g, 8), :] = pltpu.roll(scale, turn, 1)[:, :SHARE]

    def turned(t, pair, j, scaled):
        blocks = []
        for h in range(2):
            e = pair * 2 + h
            rows = pl.ds(pl.multiple_of(e * ROWS, ROWS), ROWS)
            block = fresh[t, rows, j * 128 : j * 128 + 128]
            if scaled:
                block = block * inverse[t, 2 * j + e // 8, pl.ds(lax.rem(e, 8), 1), :]
            blocks.append(block)
        return jnp.concatenate(blocks, axis=0).T

    def early_unit(u):
        for j in range(8):
            early_out[u, j * 128 : j * 128 + 128, :] = turned(0, u, j, False)
        early_in[u, me] = early_out[u, pl.ds(pl.multiple_of(me * SHARE, SHARE), SHARE), :]

    def early_send_to(u, group):
        for peer in group:
            pltpu.make_async_remote_copy(
                early_out.at[u, pl.ds(pl.multiple_of(peer * SHARE, SHARE), SHARE)],
                early_in.at[u, me], early_send.at[u], early_recv.at[u],
                device_id={"zero": peer}, device_id_type=MESH,
            ).start()

    def bulk_unit(t, pair, order):
        u = t * 8 + pair
        for j in range(8):
            narrow[u, j * 128 : j * 128 + 128, :] = turned(t, pair, j, True).astype(BF16)
        for peer in order:
            pltpu.make_async_remote_copy(
                narrow.at[u, pl.ds(pl.multiple_of(peer * SHARE, SHARE), SHARE)],
                landed.at[u, me], bulk_send.at[u], bulk_recv.at[u],
                device_id={"zero": peer}, device_id_type=MESH,
            ).start()
        landed[u, me] = narrow[u, pl.ds(pl.multiple_of(me * SHARE, SHARE), SHARE), :]

    def bulk(t, start, stop):
        def step(pair, carry):
            bulk_unit(t, pair, peers)
            return carry

        lax.fori_loop(start, stop, step, 0)

    mean(0, 0, 1)
    if EARLY:
        early_unit(0)
    mean(0, 1, 4)
    pl.semaphore_wait(barrier, len(plane) + len(nearby))
    share_parts(0)
    slot = bank * 2 + half
    for to_bank, to_zero in nearby:
        pltpu.make_async_remote_copy(
            near_out, near_in.at[slot], near_sem.at[0], near_sem.at[1],
            device_id={"bank": to_bank, "zero": to_zero}, device_id_type=MESH,
        ).start()
    near_in[slot] = near_out[...]
    if EARLY:
        early_send_to(0, plane)
    mean(1)
    share_totals(0)
    share_parts(1)
    for u in range(EARLY):
        if u:
            early_unit(u)
            early_send_to(u, plane)
        early_send_to(u, across)

    wait_for(near_in.at[pl.ds(0, 7)], near_sem.at[1])
    low = lax.broadcasted_iota(jnp.int32, (16, 128), 1) < 64
    for b in range(4):
        even, odd = near_in[2 * b].astype(F32), near_in[2 * b + 1].astype(F32)
        far_out[pl.ds(16 * b, 16), :] = jnp.where(low, even, odd).astype(BF16)
    for offset, peer in zip(ORDER, peers):
        if offset[0] == 0:
            pltpu.make_async_remote_copy(
                far_out, far_in.at[me // 2], far_sem.at[0], far_sem.at[1],
                device_id={"zero": peer}, device_id_type=MESH,
            ).start()
    far_in[me // 2] = far_out[...]

    take_totals(0, out_scale_gate)
    bulk(0, EARLY, EARLY + 2)
    share_totals(1)
    bulk(0, EARLY + 2, 8)
    take_totals(1, out_scale_up)
    bulk(1, 0, 7)
    bulk_unit(1, 7, far_first)

    wait_for(far_in.at[pl.ds(0, 15)], far_sem.at[1])
    for k in range(16):
        out_router[:, k * 128 : k * 128 + 128] = far_in[k]

    if EARLY:
        square[...] = jnp.zeros_like(square)
        square[0:8, :] = inverse[0, 2 * (me // 4)]
        columns[...] = square[...].T
        mine = columns[pl.ds(pl.multiple_of(SHARE * lax.rem(me, 4), SHARE), SHARE), :]
    for u in range(EARLY):
        wait_for(early_in.at[u, pl.ds(0, PEERS - 1)], early_recv.at[u])
        for k in range(16):
            even, odd = early_in[u, 2 * k], early_in[u, 2 * k + 1]
            to = slice(k * 128, k * 128 + 128)
            for h, lanes in ((0, slice(0, 64)), (1, slice(64, 128))):
                e = 2 * u + h
                row = jnp.concatenate([even[:, lanes], odd[:, lanes]], axis=1)
                out_gate[e, :, to] = (row * mine[:, e : e + 1]).astype(BF16)

    for t, out in ((0, out_gate), (1, out_up)):

        def place_step(pair, carry, t=t, out=out):
            u = t * 8 + pair
            wait_for(landed.at[u, pl.ds(0, PEERS - 1)], bulk_recv.at[u])
            for k in range(16):
                even, odd = landed[u, 2 * k], landed[u, 2 * k + 1]
                to = slice(k * 128, k * 128 + 128)
                out[pair * 2, :, to] = jnp.concatenate([even[:, :64], odd[:, :64]], axis=1)
                out[pair * 2 + 1, :, to] = jnp.concatenate([even[:, 64:], odd[:, 64:]], axis=1)
            return carry

        lax.fori_loop(EARLY * (1 - t), 8, place_step, 0)

    for u in range(EARLY):
        wait_for(early_in.at[u, pl.ds(0, PEERS - 1)], early_send.at[u])
    for u in range(EARLY, 16):
        wait_for(landed.at[u, pl.ds(0, PEERS - 1)], bulk_send.at[u])
    for t in range(2):
        wait_for(part_in.at[t, pl.ds(0, 15)], part_send.at[t])
    wait_for(near_in.at[pl.ds(0, 7)], near_sem.at[0])
    wait_for(far_in.at[pl.ds(0, 15)], far_sem.at[0])


def write_out(*refs):
    sources, targets, sems = refs[:5], refs[5:10], refs[10]
    copies = [pltpu.make_async_copy(*pair, sems.at[n]) for n, pair in enumerate(zip(sources, targets))]
    for copy in copies:
        copy.start()
    for copy in copies:
        copy.wait()


def on_device(w_gate, avg_gate, w_up, avg_up, mix_share, router_weight, router_gain):
    flat = [a.reshape(EXPERTS * ROWS, WIDTH) for a in (w_gate, avg_gate, w_up, avg_up)]
    vmem = pl.BlockSpec(memory_space=pltpu.VMEM)
    results = (
        ((EXPERTS, SHARE, D_MODEL), BF16),
        ((EXPERTS, SHARE, D_MODEL), BF16),
        ((EXPERTS, SHARE), F32),
        ((EXPERTS, SHARE), F32),
        ((4 * EXPERTS, D_MODEL), BF16),
    )
    held = pl.pallas_call(
        kernel,
        out_shape=tuple(pltpu.VMEM(*r) for r in results),
        in_specs=[pl.BlockSpec(memory_space=pltpu.SMEM), vmem, vmem]
        + [pl.BlockSpec(memory_space=pltpu.HBM)] * 4,
        out_specs=(vmem,) * 5,
        scratch_shapes=[
            pltpu.VMEM((2, EXPERTS * ROWS, WIDTH), F32),
            pltpu.VMEM((2, EXPERTS * ROWS, WIDTH), F32),
            pltpu.VMEM((2, 16, 8, 128), F32),
            pltpu.VMEM((2, 16, 8, 128), F32),
            pltpu.VMEM((2, PEERS, 8, 128), F32),
            pltpu.VMEM((2, 16, 8, 128), F32),
            pltpu.VMEM((128, 128), F32),
            pltpu.VMEM((128, 128), F32),
            pltpu.VMEM((max(EARLY, 1), WIDTH, 128), F32),
            pltpu.VMEM((max(EARLY, 1), PEERS, SHARE, 128), F32),
            pltpu.VMEM((16, WIDTH, 128), BF16),
            pltpu.VMEM((16, PEERS, SHARE, 128), BF16),
            pltpu.VMEM((16, 128), BF16),
            pltpu.VMEM((8, 16, 128), BF16),
            pltpu.VMEM((64, 128), BF16),
            pltpu.VMEM((16, 64, 128), BF16),
            pltpu.SemaphoreType.DMA((16,)),
            pltpu.SemaphoreType.DMA((2,)),
            pltpu.SemaphoreType.DMA((2,)),
            pltpu.SemaphoreType.DMA((2,)),
            pltpu.SemaphoreType.DMA((2,)),
            pltpu.SemaphoreType.DMA((max(EARLY, 1),)),
            pltpu.SemaphoreType.DMA((max(EARLY, 1),)),
            pltpu.SemaphoreType.DMA((16,)),
            pltpu.SemaphoreType.DMA((16,)),
            pltpu.SemaphoreType.DMA((2,)),
            pltpu.SemaphoreType.DMA((2,)),
        ],
        compiler_params=pltpu.CompilerParams(
            collective_id=0, has_side_effects=True, vmem_limit_bytes=58 * 1024 * 1024
        ),
        name="exchange",
    )(mix_share, router_weight.T, router_gain.reshape(1, ROWS), *flat)
    gate, up, scale_gate, scale_up, router = pl.pallas_call(
        write_out,
        out_shape=tuple(pltpu.HBM(*r) for r in results),
        in_specs=[vmem] * len(results),
        out_specs=(pl.BlockSpec(memory_space=pltpu.HBM),) * len(results),
        scratch_shapes=[pltpu.SemaphoreType.DMA((len(results),))],
        compiler_params=pltpu.CompilerParams(vmem_limit_bytes=16 * 1024 * 1024),
        name="write_out",
    )(*(pltpu.with_memory_space_constraint(a, pltpu.VMEM) for a in held))
    return (
        jnp.swapaxes(gate, 1, 2),
        jnp.swapaxes(up, 1, 2),
        scale_gate,
        scale_up,
        router.T,
    )


def solution(mesh):
    in_specs = (
        P("bank", "zero", None),
        P("bank", "zero", None),
        P("bank", "zero", None),
        P("bank", "zero", None),
        P("bank"),
        P("zero", "bank"),
        P("zero"),
    )
    out_specs = (
        P("bank", None, "zero"),
        P("bank", None, "zero"),
        P("bank", "zero"),
        P("bank", "zero"),
        P(),
    )
    return jax.shard_map(
        on_device, mesh=mesh, in_specs=in_specs, out_specs=out_specs, check_vma=False
    )
```

```python
import functools

import jax
import jax.numpy as jnp
from jax import lax
from jax.experimental import pallas as pl
from jax.experimental.pallas import tpu as pltpu
from jax.sharding import PartitionSpec as P

D_MODEL = 2048
EXPERTS = 16
ROWS = 64
WIDTH = 1024
PEERS = 32
SHARE = 32
EARLY = 1
BEFORE = 2
F32 = jnp.float32
BF16 = jnp.bfloat16
MESH = pl.DeviceIdType.MESH


def peer_order():
    every = [(x, y, z) for z in range(4) for y in range(4) for x in range(2)][1:]
    along_x = [o for o in every if o[0]]
    along_y = [o for o in every if not o[0] and o[1]]
    along_z = [o for o in every if not o[0] and not o[1]]
    order = []
    while along_x or along_y or along_z:
        if along_x:
            order.append(along_x.pop(0))
        if along_y:
            order.append(along_y.pop(0))
        if along_z and (len(order) % 3 == 0 or not (along_x or along_y)):
            order.append(along_z.pop(0))
    return order


ORDER = peer_order()
FAR_FIRST = sorted(ORDER, key=lambda o: -(2 * o[0] + min(o[1], 4 - o[1]) + min(o[2], 4 - o[2])))


def place(me, offset):
    x, y, z = offset
    at_z = lax.rem(me // 8 + z, 4)
    at_y = lax.rem(lax.rem(me // 2, 4) + y, 4)
    at_x = lax.rem(lax.rem(me, 2) + x, 2)
    return at_z * 8 + at_y * 2 + at_x


def wait_for(ref, sem):
    pltpu.make_async_copy(ref, ref, sem).wait()


def kernel(
    mix_ref,
    router_ref,
    gain_ref,
    w_gate,
    avg_gate,
    w_up,
    avg_up,
    out_gate,
    out_up,
    out_scale_gate,
    out_scale_up,
    out_router,
    fresh,
    other,
    part,
    part_in,
    total,
    inverse,
    square,
    columns,
    early_out,
    early_in,
    narrow,
    landed,
    near_out,
    near_in,
    far_out,
    far_in,
    load_sem,
    part_send,
    part_recv,
    total_send,
    total_recv,
    early_send,
    early_recv,
    bulk_send,
    bulk_recv,
    near_sem,
    far_sem,
    swap_sem,
):
    me = lax.axis_index("zero")
    bank = lax.axis_index("bank")
    half = lax.rem(me, 2)
    barrier = pltpu.get_barrier_semaphore()
    peers = [place(me, o) for o in ORDER]
    far_first = [place(me, o) for o in FAR_FIRST]
    nearby = [
        (lax.rem(bank + b, 4), me + h * (1 - 2 * half))
        for b in range(4)
        for h in range(2)
        if (b, h) != (0, 0)
    ]
    for peer in far_first:
        pl.semaphore_signal(barrier, inc=1, device_id={"zero": peer}, device_id_type=MESH)
    for to_bank, to_zero in nearby:
        pl.semaphore_signal(
            barrier, inc=1, device_id={"bank": to_bank, "zero": to_zero}, device_id_type=MESH
        )

    loads = []
    for t, (w, a) in enumerate(((w_gate, avg_gate), (w_up, avg_up))):
        for q in range(4):
            rows = pl.ds(q * 256, 256)
            for n, (source, target) in enumerate(((w, fresh), (a, other))):
                copy = pltpu.make_async_copy(
                    source.at[rows], target.at[t, rows], load_sem.at[t * 8 + q * 2 + n]
                )
                copy.start()
                loads.append(copy)

    share = router_ref[...] * gain_ref[...]
    near_out[...] = jnp.concatenate([share, share], axis=1).astype(BF16)

    def mean(t, first=0, last=4):
        for q in range(first, last):
            for copy in loads[t * 8 + q * 2 : t * 8 + q * 2 + 2]:
                copy.wait()

            def mean_step(n, carry, q=q):
                e = q * 4 + n
                mix = mix_ref[e]
                rest = 1.0 - mix
                rows = pl.ds(pl.multiple_of(e * ROWS, ROWS), ROWS)
                for c in range(8):
                    lanes = slice(c * 128, c * 128 + 128)
                    value = mix * fresh[t, rows, lanes] + rest * other[t, rows, lanes]
                    fresh[t, rows, lanes] = value
                    part[t, 4 * c + q, pl.ds(n, 1), :] = jnp.sum(
                        jnp.abs(value), axis=0, keepdims=True
                    )
                return carry

            lax.fori_loop(0, 4, mean_step, 0)

    def share_parts(t):
        for peer in far_first:
            pltpu.make_async_remote_copy(
                part.at[t, peer], part_in.at[t, me], part_send.at[t], part_recv.at[t],
                device_id={"zero": peer}, device_id_type=MESH,
            ).start()
        part_in[t, me] = part[t, me]

    def share_totals(t):
        wait_for(part_in.at[t, pl.ds(0, PEERS - 1)], part_recv.at[t])
        summed = part_in[t, 0]
        for n in range(1, PEERS):
            summed = summed + part_in[t, n]
        total[t, me] = summed
        for peer in far_first:
            pltpu.make_async_remote_copy(
                total.at[t, me], total.at[t, me], total_send.at[t], total_recv.at[t],
                device_id={"zero": peer}, device_id_type=MESH,
            ).start()

    def take_totals(t):
        wait_for(total.at[t, pl.ds(0, PEERS - 1)], total_recv.at[t])
        for n in range(PEERS):
            inverse[t, n] = 1.0 / (total[t, n] / D_MODEL)

    def give_scales(t, out):
        wait_for(total.at[t, pl.ds(0, PEERS - 1)], total_send.at[t])
        turn = lax.rem(128 - SHARE * lax.rem(me, 4), 128)
        for g in range(4):
            tile = total[t, 4 * (me // 4) + g] / D_MODEL
            out[pl.ds(4 * g, 4), :] = pltpu.roll(tile, turn, 1)[:, :SHARE]

    def turned(t, pair, j, scaled):
        blocks = []
        for h in range(2):
            e = pair * 2 + h
            rows = pl.ds(pl.multiple_of(e * ROWS, ROWS), ROWS)
            block = fresh[t, rows, j * 128 : j * 128 + 128]
            if scaled:
                block = block * inverse[t, 4 * j + e // 4, pl.ds(lax.rem(e, 4), 1), :]
            blocks.append(block)
        return jnp.concatenate(blocks, axis=0).T

    def early_unit(u):
        for j in range(8):
            early_out[u, j * 128 : j * 128 + 128, :] = turned(0, u, j, False)
        early_in[u, me] = early_out[u, pl.ds(pl.multiple_of(me * SHARE, SHARE), SHARE), :]

    def early_piece(u, h):
        for peer in peers:
            pltpu.make_async_remote_copy(
                early_out.at[u, pl.ds(pl.multiple_of(peer * SHARE + h * 8, 8), 8)],
                early_in.at[u, me, pl.ds(h * 8, 8)],
                early_send.at[4 * u + h], early_recv.at[4 * u + h],
                device_id={"zero": peer}, device_id_type=MESH,
            ).start()

    def bulk_unit(t, pair, order):
        u = t * 8 + pair
        for j in range(8):
            narrow[u, j * 128 : j * 128 + 128, :] = turned(t, pair, j, True).astype(BF16)
        for peer in order:
            pltpu.make_async_remote_copy(
                narrow.at[u, pl.ds(pl.multiple_of(peer * SHARE, SHARE), SHARE)],
                landed.at[u, me], bulk_send.at[u], bulk_recv.at[u],
                device_id={"zero": peer}, device_id_type=MESH,
            ).start()
        landed[u, me] = narrow[u, pl.ds(pl.multiple_of(me * SHARE, SHARE), SHARE), :]

    def bulk(t, start, stop):
        def step(pair, carry):
            bulk_unit(t, pair, peers)
            return carry

        lax.fori_loop(start, stop, step, 0)

    mean(0, 0, 1)
    if EARLY:
        early_unit(0)
    mean(0, 1, 4)
    pl.semaphore_wait(barrier, len(peers) + len(nearby))
    share_parts(0)
    slot = bank * 2 + half
    for to_bank, to_zero in nearby:
        pltpu.make_async_remote_copy(
            near_out, near_in.at[slot], near_sem.at[0], near_sem.at[1],
            device_id={"bank": to_bank, "zero": to_zero}, device_id_type=MESH,
        ).start()
    near_in[slot] = near_out[...]
    pieces = [(u, h) for u in range(EARLY) for h in range(4)]
    for piece in pieces[:BEFORE]:
        early_piece(*piece)
    mean(1)
    share_totals(0)
    share_parts(1)
    for u in range(1, EARLY):
        early_unit(u)
    for piece in pieces[BEFORE:]:
        early_piece(*piece)

    wait_for(near_in.at[pl.ds(0, 7)], near_sem.at[1])
    low = lax.broadcasted_iota(jnp.int32, (16, 128), 1) < 64
    for b in range(4):
        even, odd = near_in[2 * b].astype(F32), near_in[2 * b + 1].astype(F32)
        far_out[pl.ds(16 * b, 16), :] = jnp.where(low, even, odd).astype(BF16)
    core = lax.rem(bank, 2)
    own_rows = pl.ds(pl.multiple_of(32 * core, 32), 32)
    for offset, peer in zip(ORDER, peers):
        if offset[0] == 0:
            pltpu.make_async_remote_copy(
                far_out.at[own_rows], far_in.at[me // 2, own_rows], far_sem.at[0], far_sem.at[1],
                device_id={"zero": peer}, device_id_type=MESH,
            ).start()
    far_in[me // 2, own_rows, :] = far_out[own_rows, :]

    take_totals(0)
    bulk(0, EARLY, EARLY + 2)
    share_totals(1)
    bulk(0, EARLY + 2, 8)
    take_totals(1)
    bulk(1, 0, 7)
    bulk_unit(1, 7, far_first)
    give_scales(0, out_scale_gate)
    give_scales(1, out_scale_up)

    wait_for(far_in.at[pl.ds(0, 15), pl.ds(0, 32)], far_sem.at[1])
    pltpu.make_async_remote_copy(
        far_in.at[:, own_rows], far_in.at[:, own_rows], swap_sem.at[0], swap_sem.at[1],
        device_id={"bank": bank + 1 - 2 * core, "zero": me}, device_id_type=MESH,
    ).start()
    wait_for(far_in.at[:, pl.ds(0, 32)], swap_sem.at[1])
    for k in range(16):
        out_router[:, k * 128 : k * 128 + 128] = far_in[k]

    if EARLY:
        square[...] = jnp.zeros_like(square)
        square[0:4, :] = inverse[0, 4 * (me // 4)]
        columns[...] = square[...].T
        mine = columns[pl.ds(pl.multiple_of(SHARE * lax.rem(me, 4), SHARE), SHARE), :]
    for u in range(EARLY):
        for h in range(4):
            wait_for(early_in.at[u, pl.ds(0, PEERS - 1), pl.ds(0, 8)], early_recv.at[4 * u + h])
        for k in range(16):
            even, odd = early_in[u, 2 * k], early_in[u, 2 * k + 1]
            to = slice(k * 128, k * 128 + 128)
            for h, lanes in ((0, slice(0, 64)), (1, slice(64, 128))):
                e = 2 * u + h
                row = jnp.concatenate([even[:, lanes], odd[:, lanes]], axis=1)
                out_gate[e, :, to] = (row * mine[:, e : e + 1]).astype(BF16)

    for t, out in ((0, out_gate), (1, out_up)):

        def place_step(pair, carry, t=t, out=out):
            u = t * 8 + pair
            wait_for(landed.at[u, pl.ds(0, PEERS - 1)], bulk_recv.at[u])
            for k in range(16):
                even, odd = landed[u, 2 * k], landed[u, 2 * k + 1]
                to = slice(k * 128, k * 128 + 128)
                out[pair * 2, :, to] = jnp.concatenate([even[:, :64], odd[:, :64]], axis=1)
                out[pair * 2 + 1, :, to] = jnp.concatenate([even[:, 64:], odd[:, 64:]], axis=1)
            return carry

        lax.fori_loop(EARLY * (1 - t), 8, place_step, 0)

    for u, h in pieces:
        wait_for(early_in.at[u, pl.ds(0, PEERS - 1), pl.ds(0, 8)], early_send.at[4 * u + h])
    for u in range(EARLY, 16):
        wait_for(landed.at[u, pl.ds(0, PEERS - 1)], bulk_send.at[u])
    for t in range(2):
        wait_for(part_in.at[t, pl.ds(0, PEERS - 1)], part_send.at[t])
    wait_for(near_in.at[pl.ds(0, 7)], near_sem.at[0])
    wait_for(far_in.at[pl.ds(0, 15), pl.ds(0, 32)], far_sem.at[0])
    wait_for(far_in.at[:, pl.ds(0, 32)], swap_sem.at[0])


def write_out(*refs):
    sources, targets, sems = refs[:5], refs[5:10], refs[10]
    copies = [pltpu.make_async_copy(*pair, sems.at[n]) for n, pair in enumerate(zip(sources, targets))]
    for copy in copies:
        copy.start()
    for copy in copies:
        copy.wait()


def on_device(w_gate, avg_gate, w_up, avg_up, mix_share, router_weight, router_gain):
    flat = [a.reshape(EXPERTS * ROWS, WIDTH) for a in (w_gate, avg_gate, w_up, avg_up)]
    vmem = pl.BlockSpec(memory_space=pltpu.VMEM)
    results = (
        ((EXPERTS, SHARE, D_MODEL), BF16),
        ((EXPERTS, SHARE, D_MODEL), BF16),
        ((EXPERTS, SHARE), F32),
        ((EXPERTS, SHARE), F32),
        ((4 * EXPERTS, D_MODEL), BF16),
    )
    held = pl.pallas_call(
        kernel,
        out_shape=tuple(pltpu.VMEM(*r) for r in results),
        in_specs=[pl.BlockSpec(memory_space=pltpu.SMEM), vmem, vmem]
        + [pl.BlockSpec(memory_space=pltpu.HBM)] * 4,
        out_specs=(vmem,) * 5,
        scratch_shapes=[
            pltpu.VMEM((2, EXPERTS * ROWS, WIDTH), F32),
            pltpu.VMEM((2, EXPERTS * ROWS, WIDTH), F32),
            pltpu.VMEM((2, PEERS, 4, 128), F32),
            pltpu.VMEM((2, PEERS, 4, 128), F32),
            pltpu.VMEM((2, PEERS, 4, 128), F32),
            pltpu.VMEM((2, PEERS, 4, 128), F32),
            pltpu.VMEM((128, 128), F32),
            pltpu.VMEM((128, 128), F32),
            pltpu.VMEM((max(EARLY, 1), WIDTH, 128), F32),
            pltpu.VMEM((max(EARLY, 1), PEERS, SHARE, 128), F32),
            pltpu.VMEM((16, WIDTH, 128), BF16),
            pltpu.VMEM((16, PEERS, SHARE, 128), BF16),
            pltpu.VMEM((16, 128), BF16),
            pltpu.VMEM((8, 16, 128), BF16),
            pltpu.VMEM((64, 128), BF16),
            pltpu.VMEM((16, 64, 128), BF16),
            pltpu.SemaphoreType.DMA((16,)),
            pltpu.SemaphoreType.DMA((2,)),
            pltpu.SemaphoreType.DMA((2,)),
            pltpu.SemaphoreType.DMA((2,)),
            pltpu.SemaphoreType.DMA((2,)),
            pltpu.SemaphoreType.DMA((max(4 * EARLY, 1),)),
            pltpu.SemaphoreType.DMA((max(4 * EARLY, 1),)),
            pltpu.SemaphoreType.DMA((16,)),
            pltpu.SemaphoreType.DMA((16,)),
            pltpu.SemaphoreType.DMA((2,)),
            pltpu.SemaphoreType.DMA((2,)),
            pltpu.SemaphoreType.DMA((2,)),
        ],
        compiler_params=pltpu.CompilerParams(
            collective_id=0, has_side_effects=True, vmem_limit_bytes=58 * 1024 * 1024
        ),
        name="exchange",
    )(mix_share, router_weight.T, router_gain.reshape(1, ROWS), *flat)
    gate, up, scale_gate, scale_up, router = pl.pallas_call(
        write_out,
        out_shape=tuple(pltpu.HBM(*r) for r in results),
        in_specs=[vmem] * len(results),
        out_specs=(pl.BlockSpec(memory_space=pltpu.HBM),) * len(results),
        scratch_shapes=[pltpu.SemaphoreType.DMA((len(results),))],
        compiler_params=pltpu.CompilerParams(vmem_limit_bytes=16 * 1024 * 1024),
        name="write_out",
    )(*(pltpu.with_memory_space_constraint(a, pltpu.VMEM) for a in held))
    return (
        jnp.swapaxes(gate, 1, 2),
        jnp.swapaxes(up, 1, 2),
        scale_gate,
        scale_up,
        router.T,
    )


def solution(mesh):
    in_specs = (
        P("bank", "zero", None),
        P("bank", "zero", None),
        P("bank", "zero", None),
        P("bank", "zero", None),
        P("bank"),
        P("zero", "bank"),
        P("zero"),
    )
    out_specs = (
        P("bank", None, "zero"),
        P("bank", None, "zero"),
        P("bank", "zero"),
        P("bank", "zero"),
        P(),
    )
    return jax.shard_map(
        on_device, mesh=mesh, in_specs=in_specs, out_specs=out_specs, check_vma=False
    )
```
